32 devices in a mesh: freq: 4 (over y, x), space: 8 (over z, core).
Axes of the slice: x: 2, y: 2, z: 4, core: 2. Of those that a mesh axis runs over, the one named last changes fastest.
Arguments:
- spectra: bfloat16 [64, 24576, 256], P('freq', 'space'), may hold values from -48 to 48, as said below
- weight: float32 [24576], P('space'), may hold values from 0.25 to 4
- partner: int32 [64], P('freq'), may hold values from 0 to 15
- counts: int32 [64], P('freq'), may hold values from 1 to 8
Outputs:
- modes: bfloat16 [64, 16, 24576], P('freq', None, 'space')
- energy: float32 [64, 8], P('freq')
- coherence: float32 [64, 2, 8, 8], P('freq')
The draws below stay inside these ranges and needn't reach their ends.
Inputs may be any that keep to these rules, and one draw needn't show every extreme that they name: spectra are finite Fourier coefficients.
All inputs are finite; a program needn't handle non-finite values.
Results may differ from the reference program's by a relative error of at most 0.0045.
Values may be sent and summed in bfloat16 or wider, within the bound.
A program may use at most 128 MiB of HBM per device.

```python
import math
import jax
import jax.numpy as jnp
from jax import lax

NB = 128
FG = 16
KMAX = 8
ITERS = 4
NF = 64
NP = 24576
N_FREQ = 4


shared_terms = 256


def draw_spectra(key, part):
    keys = jax.random.split(key, 4)
    scales = jnp.exp(jax.random.uniform(keys[0], (NF, 1, NB), jnp.float32, 0.0, math.log(4.0)))
    noise = jax.random.normal(keys[1], (NF, NP, 2 * NB), jnp.float32)
    amplitude = 0.6
    shared = jax.random.normal(keys[2], (NP, shared_terms), jnp.float32)
    mixing = jax.random.normal(keys[3], (NF, shared_terms, 2 * NB), jnp.float32) * (amplitude * math.sqrt(8.0 / shared_terms))
    common = jnp.einsum('pr,frc->fpc', shared, mixing)
    doubled = jnp.concatenate([scales, scales], axis=2)
    return jnp.clip(doubled * (noise + common), -48.0, 48.0).astype(jnp.bfloat16)


def touch_ends(result, rng, low, high):
    place = [jax.random.randint(jax.random.fold_in(rng, axis), (), 0, length) for axis, length in enumerate(result.shape)]
    longest = result.shape.index(max(result.shape))
    beside = place[:longest] + [(place[longest] + 1) % result.shape[longest]] + place[longest + 1:]
    return result.at[tuple(place)].set(low).at[tuple(beside)].set(high)


def block_scale(rng, shape, cuts, smallest, high):
    loudness = 1.0
    for position, shards_of in cuts:
        heights = jax.random.uniform(jax.random.fold_in(jax.random.fold_in(rng, 6), position), (shards_of,), jnp.float32, smallest / len(cuts), high / len(cuts))
        loudness = loudness * jnp.repeat(jnp.exp(heights), shape[position] // shards_of).reshape((-1,) + (1,) * (len(shape) - 1 - position))
    return loudness


def setup_inputs(seed: int = 0) -> dict:
    arg_keys = jax.random.split(jax.random.key(seed), 5)
    return {
        "spectra": draw_spectra(jax.random.fold_in(arg_keys[4], 71), 0),
        "weight": jnp.clip(jnp.exp(math.log(4.0) - 2.7725887 * jax.random.uniform(arg_keys[1], (NP,), jnp.float32) ** block_scale(arg_keys[1], (NP,), ((0, 8),), -0.2, 0.2)), 0.25, 4.0),
        "partner": touch_ends(jax.random.randint(arg_keys[2], (NF,), 0, FG), jax.random.fold_in(arg_keys[2], 1), 0, FG - 1).astype(jnp.int32),
        "counts": touch_ends(jax.random.randint(arg_keys[3], (NF,), 1, KMAX + 1), jax.random.fold_in(arg_keys[3], 1), 1, KMAX).astype(jnp.int32),
    }


def embed(gram_re, gram_im):
    top = jnp.concatenate([gram_re, -gram_im], axis=2)
    bottom = jnp.concatenate([gram_im, gram_re], axis=2)
    return jnp.concatenate([top, bottom], axis=1)

def apply_operator(operator, basis):
    return jnp.einsum('fkc,fdc->fkd', basis, operator, precision=lax.Precision.HIGHEST)

def orthonormal(vectors, half):
    done = []
    for index in range(vectors.shape[1]):
        vector = vectors[:, index, :]
        for earlier in done:
            early_re, early_im = (earlier[:, :half], earlier[:, half:])
            vec_re, vec_im = (vector[:, :half], vector[:, half:])
            proj_re = lax.optimization_barrier(jnp.sum(early_re * vec_re + early_im * vec_im, axis=1, keepdims=True))
            proj_im = lax.optimization_barrier(jnp.sum(early_re * vec_im - early_im * vec_re, axis=1, keepdims=True))
            new_re = vec_re - proj_re * early_re + proj_im * early_im
            new_im = vec_im - proj_re * early_im - proj_im * early_re
            vector = jnp.concatenate([new_re, new_im], axis=1)
        length = jnp.sqrt(lax.optimization_barrier(jnp.sum(vector * vector, axis=1, keepdims=True)) + 1e-06)
        done.append(vector / length)
    return jnp.stack(done, axis=1)

def solve(gram_re, gram_im):
    half = gram_re.shape[1]
    operator = embed(gram_re, gram_im)
    basis = jnp.broadcast_to(jnp.eye(KMAX, 2 * half, dtype=jnp.float32), (gram_re.shape[0], KMAX, 2 * half))
    for sweep in range(ITERS):
        basis = orthonormal(apply_operator(operator, basis), half)
    image = apply_operator(operator, basis)
    energy = lax.optimization_barrier(jnp.sum(basis * image, axis=2))
    return (basis, energy)

def coefficients(basis, energy, counts):
    half = basis.shape[2] // 2
    ranks = jnp.arange(KMAX, dtype=jnp.int32)[None, :]
    scale = jnp.where(ranks < counts[:, None], 1.0 / jnp.sqrt(energy + 1e-06), 0.0)[:, :, None]
    part_re, part_im = (basis[:, :, :half], basis[:, :, half:])
    upper = jnp.concatenate([part_re, -part_im], axis=2) * scale
    lower = jnp.concatenate([part_im, part_re], axis=2) * scale
    return jnp.concatenate([upper, lower], axis=1).astype(jnp.bfloat16)

def reference(spectra, weight, partner, counts):
    half = NB

    def moment(block):
        weighted = (weight[:, None] * block).astype(jnp.bfloat16)
        return jnp.dot(block.T, weighted, preferred_element_type=jnp.float32)
    moments = lax.map(moment, spectra)
    gram_re = (moments[:, :half, :half] + moments[:, half:, half:]) / NP
    gram_im = (moments[:, :half, half:] - moments[:, half:, :half]) / NP
    basis, energy = solve(gram_re, gram_im)
    coefficient = coefficients(basis, energy, counts)

    def project(pair):
        return jnp.dot(pair[0], pair[1].T, preferred_element_type=jnp.float32).astype(jnp.bfloat16)
    modes = lax.map(project, (coefficient, spectra))
    freqs = jnp.arange(NF, dtype=jnp.int32)
    source = (N_FREQ - 1 - freqs // FG) * FG + partner
    partner_modes = jnp.take(modes, source.astype(jnp.int32), axis=0)

    def cohere(pair):
        phi = pair[0].astype(jnp.float32)
        psi = pair[1].astype(jnp.float32)
        wphi = phi * weight[None, :]
        hi = lax.Precision.HIGHEST
        real_part = jnp.dot(wphi[:KMAX], psi[:KMAX].T, precision=hi) + jnp.dot(wphi[KMAX:], psi[KMAX:].T, precision=hi)
        imag_part = jnp.dot(wphi[:KMAX], psi[KMAX:].T, precision=hi) - jnp.dot(wphi[KMAX:], psi[:KMAX].T, precision=hi)
        return jnp.stack([real_part, imag_part], axis=0) / NP
    coherence = lax.map(cohere, (modes, partner_modes))
    return (modes, energy, coherence)
```

```python
import functools

import jax
import jax.numpy as jnp
from jax import lax
from jax.experimental import pallas as pl
from jax.experimental.pallas import tpu as pltpu
from jax.sharding import PartitionSpec as P

KMAX = 8
ITERS = 4
AHEAD = 4
LINK = jnp.bfloat16
MESH = pl.DeviceIdType.MESH
F32 = jnp.float32
BF16 = jnp.bfloat16


def dot(left, right, dims, precision=None):
    return lax.dot_general(
        left, right, (dims, ((), ())), precision=precision, preferred_element_type=F32
    )


def split(value):
    high = value.astype(BF16)
    return high, (value - high.astype(F32)).astype(BF16)


def pack(moments, half):
    real = moments[:half, :half] + moments[half:, half:]
    imag = moments[:half, half:] - moments[half:, :half]
    row = lax.broadcasted_iota(jnp.int32, (half, half), 0)
    col = lax.broadcasted_iota(jnp.int32, (half, half), 1)
    return jnp.where(row <= col, real, imag)


def unpack(packed, half):
    row = lax.broadcasted_iota(jnp.int32, (half, half), 0)
    col = lax.broadcasted_iota(jnp.int32, (half, half), 1)
    other = packed.T
    real = jnp.where(row <= col, packed, other)
    imag = jnp.where(row > col, packed, jnp.where(row < col, -other, 0.0))
    return real, imag


def orthonormal(real, imag):
    row = lax.broadcasted_iota(jnp.int32, real.shape, 0)
    for k in range(KMAX):
        a_re = jnp.broadcast_to(real[k : k + 1, :], real.shape)
        a_im = jnp.broadcast_to(imag[k : k + 1, :], imag.shape)
        norm = jnp.sum(a_re * a_re + a_im * a_im, axis=1, keepdims=True)
        p_re = jnp.sum(a_re * real + a_im * imag, axis=1, keepdims=True)
        p_im = jnp.sum(a_re * imag - a_im * real, axis=1, keepdims=True)
        inverse = 1.0 / jnp.sqrt(norm + 1e-06)
        e_re, e_im = a_re * inverse, a_im * inverse
        q_re, q_im = p_re * inverse, p_im * inverse
        later_re = real - q_re * e_re + q_im * e_im
        later_im = imag - q_re * e_im - q_im * e_re
        real = jnp.where(row > k, later_re, jnp.where(row == k, e_re, real))
        imag = jnp.where(row > k, later_im, jnp.where(row == k, e_im, imag))
    return real, imag


def apply_operator(operator, real, imag, half):
    high, low = split(jnp.concatenate([real, imag], axis=0))
    left = jnp.concatenate([high, high, low], axis=1)
    image = dot(left, operator, ((1,), (0,)))
    new_re = image[:KMAX, :half] + image[KMAX:, half:]
    new_im = image[KMAX:, :half] - image[:KMAX, half:]
    return new_re, new_im


def choose(cross, partner, groups):
    wide = 2 * KMAX * groups
    row = lax.broadcasted_iota(jnp.int32, (wide, wide), 0)
    col = lax.broadcasted_iota(jnp.int32, (wide, wide), 1)
    lane_group = col // (2 * KMAX)
    want = jnp.broadcast_to(partner[:, None, :], (groups, 2 * KMAX, partner.shape[1]))
    want = want.reshape(wide, partner.shape[1])
    kept = jnp.where(lane_group == want, cross, 0.0).reshape(groups, 2, KMAX, wide)
    top = kept[:, 0].reshape(groups * KMAX, wide)
    bottom = kept[:, 1].reshape(groups * KMAX, wide)
    from_place = row % (2 * KMAX)
    to_place = col % (2 * KMAX)
    same = jnp.where(from_place == to_place, 1.0, 0.0)
    swap = jnp.where(
        from_place == to_place + KMAX, 1.0, jnp.where(from_place == to_place - KMAX, -1.0, 0.0)
    )
    highest = lax.Precision.HIGHEST
    folded = dot(top, same, ((1,), (0,)), highest) + dot(bottom, swap, ((1,), (0,)), highest)
    shape = (groups * KMAX, wide)
    row_group = lax.broadcasted_iota(jnp.int32, shape, 0) // KMAX
    column_group = lax.broadcasted_iota(jnp.int32, shape, 1) // (2 * KMAX)
    folded = jnp.where(row_group == column_group, folded, 0.0)
    return jnp.sum(folded.reshape(groups, KMAX, wide), axis=0)


def kernel(
    n_freq, n_space, spectra, weight, partner, counts,
    modes_out, energy_out, coherence_out,
    held, columns, send, recv, message, modes, mirrored, scaled,
    partners, partials, arrived,
    load_sem, store_sem, gram_send, gram_recv, basis_send, basis_recv,
    modes_send, modes_recv, partner_send, partner_recv, part_send, part_recv,
):
    groups, points, width = held.shape
    half = width // 2
    part = points // 2
    own = groups // n_space
    total = points * n_space
    band = lax.axis_index("freq")
    me = lax.axis_index("space")
    opposite = n_freq - 1 - band
    upper = jnp.where(band > opposite, 1, 0)
    mine = pl.multiple_of(upper * part, 128)
    theirs = pl.multiple_of((1 - upper) * part, 128)

    def order(step):
        return lax.rem((me + 1) * own + step, groups)

    def load(step):
        f = order(step)
        return pltpu.make_async_copy(spectra.at[f], held.at[f], load_sem.at[f])

    for step in range(AHEAD):
        load(step).start()

    barrier = pltpu.get_barrier_semaphore()
    for apart in range(1, n_space):
        peer = lax.rem(me + apart, n_space)
        pl.semaphore_signal(barrier, inc=1, device_id=(band, peer), device_id_type=MESH)
    for apart in range(n_space):
        peer = lax.rem(me + apart, n_space)
        pl.semaphore_signal(barrier, inc=1, device_id=(opposite, peer), device_id_type=MESH)

    lane_row = lax.broadcasted_iota(jnp.int32, (groups, 128), 0)
    table = jnp.zeros((groups, 128), jnp.int32)
    for f in range(groups):
        table = jnp.where(lane_row == f, partner[f], table)
    partners[0] = table
    for block in range(points // 128):
        span = pl.ds(block * 128, 128)
        columns[span, :] = jnp.broadcast_to(weight[:, span], (128, 128)).T

    pl.semaphore_wait(barrier, 2 * n_space - 1)

    partner_copy = pltpu.make_async_remote_copy(
        src_ref=partners.at[0], dst_ref=partners.at[1], send_sem=partner_send,
        recv_sem=partner_recv, device_id=(opposite, me), device_id_type=MESH,
    )
    partner_copy.start()

    def gram_copy(f, source):
        owner = f // own
        slot = lax.rem(f, own)
        return pltpu.make_async_remote_copy(
            src_ref=send.at[f], dst_ref=recv.at[source, slot], send_sem=gram_send.at[f],
            recv_sem=gram_recv.at[source, slot], device_id=(band, owner), device_id_type=MESH,
        )

    def gram_step(step, carry):
        f = order(step)

        @pl.when(step + AHEAD < groups)
        def _():
            load(step + AHEAD).start()

        load(step).wait()
        block = held[f]
        scale = columns[...]
        weighted = (jnp.concatenate([scale, scale], axis=1) * block.astype(F32)).astype(BF16)
        packed = pack(dot(block, weighted, ((0,), (0,))), half).astype(LINK)
        owner = f // own

        @pl.when(owner != me)
        def _():
            send[f] = packed
            gram_copy(f, me).start()

        @pl.when(owner == me)
        def _():
            recv[me, lax.rem(f, own)] = packed

        return carry

    lax.fori_loop(0, groups, gram_step, 0)

    for apart in range(1, n_space):
        source = lax.rem(me + apart, n_space)
        for slot in range(own):
            gram_copy(source * own + slot, source).wait_send()
            pltpu.make_async_remote_copy(
                src_ref=send.at[0], dst_ref=recv.at[source, slot], send_sem=gram_send.at[0],
                recv_sem=gram_recv.at[source, slot], device_id=(band, source), device_id_type=MESH,
            ).wait_recv()

    operators, state = [], []
    for slot in range(own):
        packed = recv[0, slot].astype(F32)
        for source in range(1, n_space):
            packed = packed + recv[source, slot].astype(F32)
        real, imag = unpack(packed / total, half)
        high, low = split(jnp.concatenate([real, imag], axis=1))
        operators.append(jnp.concatenate([high, low, high], axis=0))
        state += [real[:KMAX], -imag[:KMAX]]

    def all_orthonormal(state):
        done = []
        for slot in range(own):
            done += orthonormal(state[2 * slot], state[2 * slot + 1])
        return tuple(done)

    def sweep(_, state):
        image = []
        for slot in range(own):
            image += apply_operator(operators[slot], state[2 * slot], state[2 * slot + 1], half)
        return all_orthonormal(image)

    state = lax.fori_loop(0, ITERS - 1, sweep, all_orthonormal(state))

    rank = lax.broadcasted_iota(jnp.int32, (KMAX, half), 0)
    for slot in range(own):
        f = me * own + slot
        real, imag = state[2 * slot], state[2 * slot + 1]
        image_re, image_im = apply_operator(operators[slot], real, imag, half)
        energy = jnp.sum(real * image_re + imag * image_im, axis=1, keepdims=True)
        energy = jnp.broadcast_to(energy, (KMAX, half))
        scale = jnp.where(rank < counts[f], 1.0 / jnp.sqrt(energy + 1e-06), 0.0)
        message[f] = jnp.concatenate([real * scale, imag * scale, energy], axis=0)

    def basis_copy(source, peer):
        span = pl.ds(source * own, own)
        return pltpu.make_async_remote_copy(
            src_ref=message.at[span], dst_ref=message.at[span], send_sem=basis_send.at[peer],
            recv_sem=basis_recv.at[source], device_id=(band, peer), device_id_type=MESH,
        )

    for apart in range(1, n_space):
        basis_copy(me, lax.rem(me + apart, n_space)).start()

    def modes_copy(f):
        return pltpu.make_async_remote_copy(
            src_ref=modes.at[f, :, pl.ds(theirs, part)], dst_ref=mirrored.at[f],
            send_sem=modes_send.at[f], recv_sem=modes_recv.at[f],
            device_id=(opposite, me), device_id_type=MESH,
        )

    def store(f):
        return pltpu.make_async_copy(modes.at[f], modes_out.at[f], store_sem.at[f])

    def modes_step(step, carry):
        f = lax.rem(me * own + step, groups)
        source = f // own

        @pl.when(jnp.logical_and(lax.rem(f, own) == 0, source != me))
        def _():
            basis_copy(source, source).wait_recv()

        basis = message[f]
        real, imag = basis[:KMAX], basis[KMAX : 2 * KMAX]
        coefficient = jnp.concatenate(
            [jnp.concatenate([real, -imag], axis=1), jnp.concatenate([imag, real], axis=1)], axis=0
        ).astype(BF16)
        modes[f] = dot(coefficient, held[f], ((1,), (1,))).astype(BF16)
        modes_copy(f).start()
        store(f).start()
        energy_out[f] = basis[2 * KMAX :]
        weighted = modes[f, :, pl.ds(mine, part)].astype(F32) * weight[:, pl.ds(mine, part)]
        high, low = split(weighted)
        scaled[0, f] = high
        scaled[1, f] = low
        return carry

    lax.fori_loop(0, groups, modes_step, 0)

    def modes_wait(f, carry):
        modes_copy(f).wait_recv()
        return carry

    partner_copy.wait()
    lax.fori_loop(0, groups, modes_wait, 0)
    wide = groups * 2 * KMAX
    psi = mirrored[...].reshape(wide, part)
    cross = dot(scaled[0].reshape(wide, part), psi, ((1,), (1,)))
    cross = (cross + dot(scaled[1].reshape(wide, part), psi, ((1,), (1,)))) / total
    spread = functools.partial(jnp.concatenate, axis=1)
    copies = wide // 128
    partials[0] = choose(cross, spread([partners[0]] * copies), groups)
    partials[1] = choose(cross.T, spread([partners[1]] * copies), groups)

    def part_copy(side, source, peer):
        across = opposite if side else band
        return pltpu.make_async_remote_copy(
            src_ref=partials.at[side], dst_ref=arrived.at[side, source],
            send_sem=part_send.at[side, peer], recv_sem=part_recv.at[side, source],
            device_id=(across, peer), device_id_type=MESH,
        )

    for apart in range(n_space):
        peer = lax.rem(me + apart, n_space)
        part_copy(1, me, peer).start()
        if apart:
            part_copy(0, me, peer).start()

    def drain(f, carry):
        modes_copy(f).wait_send()
        store(f).wait()
        return carry

    lax.fori_loop(0, groups, drain, 0)
    for apart in range(1, n_space):
        basis_copy(me, lax.rem(me + apart, n_space)).wait_send()

    result = partials[0]
    for apart in range(n_space):
        peer = lax.rem(me + apart, n_space)
        part_copy(1, peer, peer).wait()
        result = result + arrived[1, peer]
        if apart:
            part_copy(0, peer, peer).wait()
            result = result + arrived[0, peer]
    coherence_out[...] = result


def on_device(n_freq, n_space, spectra, weight, partner, counts):
    groups, points, width = spectra.shape
    half = width // 2
    own = groups // n_space
    rows = 2 * KMAX
    wide = groups * rows
    dma = pltpu.SemaphoreType.DMA
    vmem = pl.BlockSpec(memory_space=pltpu.VMEM)
    smem = pl.BlockSpec(memory_space=pltpu.SMEM)
    hbm = pl.BlockSpec(memory_space=pltpu.HBM)
    modes, energy, coherence = pl.pallas_call(
        functools.partial(kernel, n_freq, n_space),
        out_shape=(
            jax.ShapeDtypeStruct((groups, rows, points), BF16),
            jax.ShapeDtypeStruct((groups, KMAX, half), F32),
            jax.ShapeDtypeStruct((KMAX, wide), F32),
        ),
        in_specs=[hbm, vmem, smem, smem],
        out_specs=(hbm, vmem, vmem),
        scratch_shapes=[
            pltpu.VMEM((groups, points, width), BF16),
            pltpu.VMEM((points, 128), F32),
            pltpu.VMEM((groups, half, half), LINK),
            pltpu.VMEM((n_space, own, half, half), LINK),
            pltpu.VMEM((groups, 3 * KMAX, half), F32),
            pltpu.VMEM((groups, rows, points), BF16),
            pltpu.VMEM((groups, rows, points // 2), BF16),
            pltpu.VMEM((2, groups, rows, points // 2), BF16),
            pltpu.VMEM((2, groups, 128), jnp.int32),
            pltpu.VMEM((2, KMAX, wide), F32),
            pltpu.VMEM((2, n_space, KMAX, wide), F32),
            dma((groups,)),
            dma((groups,)),
            dma((groups,)),
            dma((n_space, own)),
            dma((n_space,)),
            dma((n_space,)),
            dma((groups,)),
            dma((groups,)),
            dma(()),
            dma(()),
            dma((2, n_space)),
            dma((2, n_space)),
        ],
        compiler_params=pltpu.CompilerParams(
            collective_id=0, has_side_effects=True, vmem_limit_bytes=60 * 1024 * 1024
        ),
    )(spectra, weight.reshape(1, points), partner, counts)
    coherence = coherence.reshape(KMAX, groups, 2, KMAX).transpose(1, 2, 0, 3)
    return modes, energy[:, :, 0], coherence


def solution(mesh):
    in_specs = (P("freq", "space", None), P("space"), P("freq"), P("freq"))
    out_specs = (P("freq", None, "space"), P("freq", None), P("freq", None, None, None))
    return jax.shard_map(
        functools.partial(on_device, mesh.shape["freq"], mesh.shape["space"]),
        mesh=mesh,
        in_specs=in_specs,
        out_specs=out_specs,
        check_vma=False,
    )
```

```python
import functools

import jax
import jax.numpy as jnp
from jax import lax
from jax.experimental import pallas as pl
from jax.experimental.pallas import tpu as pltpu
from jax.sharding import PartitionSpec as P

KMAX = 8
ITERS = 4
AHEAD = 4
MESH = pl.DeviceIdType.MESH
F32 = jnp.float32
BF16 = jnp.bfloat16


def dot(left, right, dims, precision=None):
    return lax.dot_general(
        left, right, (dims, ((), ())), precision=precision, preferred_element_type=F32
    )


def split(value):
    high = value.astype(BF16)
    return high, (value - high.astype(F32)).astype(BF16)


def pack(moments, half):
    real = moments[:half, :half] + moments[half:, half:]
    imag = moments[:half, half:] - moments[half:, :half]
    row = lax.broadcasted_iota(jnp.int32, (half, half), 0)
    col = lax.broadcasted_iota(jnp.int32, (half, half), 1)
    return jnp.where(row <= col, real, imag)


def unpack(packed, half):
    row = lax.broadcasted_iota(jnp.int32, (half, half), 0)
    col = lax.broadcasted_iota(jnp.int32, (half, half), 1)
    other = packed.T
    real = jnp.where(row <= col, packed, other)
    imag = jnp.where(row > col, packed, jnp.where(row < col, -other, 0.0))
    return real, imag


def orthonormal(real, imag):
    row = lax.broadcasted_iota(jnp.int32, real.shape, 0)
    for k in range(KMAX):
        a_re = jnp.broadcast_to(real[k : k + 1, :], real.shape)
        a_im = jnp.broadcast_to(imag[k : k + 1, :], imag.shape)
        norm = jnp.sum(a_re * a_re + a_im * a_im, axis=1, keepdims=True)
        p_re = jnp.sum(a_re * real + a_im * imag, axis=1, keepdims=True)
        p_im = jnp.sum(a_re * imag - a_im * real, axis=1, keepdims=True)
        inverse = 1.0 / jnp.sqrt(norm + 1e-06)
        e_re, e_im = a_re * inverse, a_im * inverse
        q_re, q_im = p_re * inverse, p_im * inverse
        later_re = real - q_re * e_re + q_im * e_im
        later_im = imag - q_re * e_im - q_im * e_re
        real = jnp.where(row > k, later_re, jnp.where(row == k, e_re, real))
        imag = jnp.where(row > k, later_im, jnp.where(row == k, e_im, imag))
    return real, imag


def apply_operator(operator, real, imag, half):
    high, low = split(jnp.concatenate([real, imag], axis=0))
    left = jnp.concatenate([high, high, low], axis=1)
    image = dot(left, operator, ((1,), (0,)))
    new_re = image[:KMAX, :half] + image[KMAX:, half:]
    new_im = image[KMAX:, :half] - image[:KMAX, half:]
    return new_re, new_im


def choose(cross, partner, groups):
    wide = 2 * KMAX * groups
    row = lax.broadcasted_iota(jnp.int32, (wide, wide), 0)
    col = lax.broadcasted_iota(jnp.int32, (wide, wide), 1)
    lane_group = col // (2 * KMAX)
    want = jnp.broadcast_to(partner[:, None, :], (groups, 2 * KMAX, partner.shape[1]))
    want = want.reshape(wide, partner.shape[1])
    kept = jnp.where(lane_group == want, cross, 0.0).reshape(groups, 2, KMAX, wide)
    top = kept[:, 0].reshape(groups * KMAX, wide)
    bottom = kept[:, 1].reshape(groups * KMAX, wide)
    from_place = row % (2 * KMAX)
    to_place = col % (2 * KMAX)
    same = jnp.where(from_place == to_place, 1.0, 0.0)
    swap = jnp.where(
        from_place == to_place + KMAX, 1.0, jnp.where(from_place == to_place - KMAX, -1.0, 0.0)
    )
    highest = lax.Precision.HIGHEST
    folded = dot(top, same, ((1,), (0,)), highest) + dot(bottom, swap, ((1,), (0,)), highest)
    shape = (groups * KMAX, wide)
    row_group = lax.broadcasted_iota(jnp.int32, shape, 0) // KMAX
    column_group = lax.broadcasted_iota(jnp.int32, shape, 1) // (2 * KMAX)
    folded = jnp.where(row_group == column_group, folded, 0.0)
    return jnp.sum(folded.reshape(groups, KMAX, wide), axis=0)


def kernel(
    n_freq, n_space, spectra, weight, partner, counts,
    modes_out, energy_out, coherence_out,
    held, columns, send, paired, recv, message, modes, mirrored, scaled,
    partners, partials, arrived,
    load_sem, store_sem, gram_send, gram_recv, mate_recv, basis_send, basis_recv,
    modes_send, modes_recv, partner_send, partner_recv, part_send, part_recv,
):
    groups, points, width = held.shape
    half = width // 2
    part = points // 2
    own = groups // n_space
    total = points * n_space
    band = lax.axis_index("freq")
    me = lax.axis_index("space")
    opposite = n_freq - 1 - band
    upper = jnp.where(band > opposite, 1, 0)
    mine = pl.multiple_of(upper * part, 128)
    theirs = pl.multiple_of((1 - upper) * part, 128)

    side = lax.rem(me, 2)
    chip = me // 2
    mate = me + 1 - 2 * side

    def order(step):
        target = lax.rem(chip + 1 + step // (2 * own), n_space // 2)
        place = lax.rem(step, 2 * own)
        parity = jnp.where(place < own, 1 - side, side)
        return (2 * target + parity) * own + lax.rem(place, own)

    def load(step):
        f = order(step)
        return pltpu.make_async_copy(spectra.at[f], held.at[f], load_sem.at[f])

    for step in range(AHEAD):
        load(step).start()

    barrier = pltpu.get_barrier_semaphore()
    for apart in range(1, n_space):
        peer = lax.rem(me + apart, n_space)
        pl.semaphore_signal(barrier, inc=1, device_id=(band, peer), device_id_type=MESH)
    for apart in range(n_space):
        peer = lax.rem(me + apart, n_space)
        pl.semaphore_signal(barrier, inc=1, device_id=(opposite, peer), device_id_type=MESH)

    lane_row = lax.broadcasted_iota(jnp.int32, (groups, 128), 0)
    table = jnp.zeros((groups, 128), jnp.int32)
    for f in range(groups):
        table = jnp.where(lane_row == f, partner[f], table)
    partners[0] = table
    for block in range(points // 128):
        span = pl.ds(block * 128, 128)
        columns[span, :] = jnp.broadcast_to(weight[:, span], (128, 128)).T

    pl.semaphore_wait(barrier, 2 * n_space - 1)

    partner_copy = pltpu.make_async_remote_copy(
        src_ref=partners.at[0], dst_ref=partners.at[1], send_sem=partner_send,
        recv_sem=partner_recv, device_id=(opposite, me), device_id_type=MESH,
    )
    partner_copy.start()

    def gram_copy(f, source):
        owner = f // own
        slot = lax.rem(f, own)
        return pltpu.make_async_remote_copy(
            src_ref=send.at[f], dst_ref=recv.at[source, slot], send_sem=gram_send.at[f],
            recv_sem=gram_recv.at[source, slot], device_id=(band, owner), device_id_type=MESH,
        )

    def mate_copy(f):
        return pltpu.make_async_remote_copy(
            src_ref=send.at[f], dst_ref=paired.at[f], send_sem=gram_send.at[f],
            recv_sem=mate_recv.at[f], device_id=(band, mate), device_id_type=MESH,
        )

    def gram_step(step, carry):
        f = order(step)

        @pl.when(step + AHEAD < groups)
        def _():
            load(step + AHEAD).start()

        load(step).wait()
        block = held[f]
        scale = columns[...]
        weighted = (jnp.concatenate([scale, scale], axis=1) * block.astype(F32)).astype(BF16)
        packed = pack(dot(block, weighted, ((0,), (0,))), half)
        owner = f // own
        same = lax.rem(owner, 2) == side

        @pl.when(jnp.logical_not(same))
        def _():
            send[f] = packed
            mate_copy(f).start()

        @pl.when(same)
        def _():
            mate_copy(f).wait_recv()
            both = packed + paired[f]

            @pl.when(owner != me)
            def _():
                send[f] = both
                gram_copy(f, chip).start()

            @pl.when(owner == me)
            def _():
                recv[chip, lax.rem(f, own)] = both

        return carry

    lax.fori_loop(0, groups, gram_step, 0)

    for apart in range(1, n_space // 2):
        source = lax.rem(chip + apart, n_space // 2)
        for slot in range(own):
            pltpu.make_async_remote_copy(
                src_ref=send.at[0], dst_ref=recv.at[source, slot], send_sem=gram_send.at[0],
                recv_sem=gram_recv.at[source, slot],
                device_id=(band, 2 * source + side), device_id_type=MESH,
            ).wait_recv()

    operators, state = [], []
    for slot in range(own):
        packed = recv[0, slot]
        for source in range(1, n_space // 2):
            packed = packed + recv[source, slot]
        real, imag = unpack(packed / total, half)
        high, low = split(jnp.concatenate([real, imag], axis=1))
        operators.append(jnp.concatenate([high, low, high], axis=0))
        state += [real[:KMAX], -imag[:KMAX]]

    def all_orthonormal(state):
        done = []
        for slot in range(own):
            done += orthonormal(state[2 * slot], state[2 * slot + 1])
        return tuple(done)

    def sweep(_, state):
        image = []
        for slot in range(own):
            image += apply_operator(operators[slot], state[2 * slot], state[2 * slot + 1], half)
        return all_orthonormal(image)

    state = lax.fori_loop(0, ITERS - 1, sweep, all_orthonormal(state))

    rank = lax.broadcasted_iota(jnp.int32, (KMAX, half), 0)
    for slot in range(own):
        f = me * own + slot
        real, imag = state[2 * slot], state[2 * slot + 1]
        image_re, image_im = apply_operator(operators[slot], real, imag, half)
        energy = jnp.sum(real * image_re + imag * image_im, axis=1, keepdims=True)
        energy = jnp.broadcast_to(energy, (KMAX, half))
        scale = jnp.where(rank < counts[f], 1.0 / jnp.sqrt(energy + 1e-06), 0.0)
        message[f] = jnp.concatenate([real * scale, imag * scale, energy], axis=0)

    def basis_copy(source, peer):
        span = pl.ds(source * own, own)
        return pltpu.make_async_remote_copy(
            src_ref=message.at[span], dst_ref=message.at[span], send_sem=basis_send.at[peer],
            recv_sem=basis_recv.at[source], device_id=(band, peer), device_id_type=MESH,
        )

    for apart in range(1, n_space):
        basis_copy(me, lax.rem(me + apart, n_space)).start()

    def modes_copy(f):
        return pltpu.make_async_remote_copy(
            src_ref=modes.at[f, :, pl.ds(theirs, part)], dst_ref=mirrored.at[f],
            send_sem=modes_send.at[f], recv_sem=modes_recv.at[f],
            device_id=(opposite, me), device_id_type=MESH,
        )

    def store(f):
        return pltpu.make_async_copy(modes.at[f], modes_out.at[f], store_sem.at[f])

    diagonal = rank == lax.broadcasted_iota(jnp.int32, (KMAX, half), 1)

    def modes_step(step, carry):
        f = lax.rem(me * own + step, groups)
        source = f // own

        @pl.when(jnp.logical_and(lax.rem(f, own) == 0, source != me))
        def _():
            basis_copy(source, source).wait_recv()

        basis = message[f]
        real, imag = basis[:KMAX], basis[KMAX : 2 * KMAX]
        coefficient = jnp.concatenate(
            [jnp.concatenate([real, -imag], axis=1), jnp.concatenate([imag, real], axis=1)], axis=0
        ).astype(BF16)
        modes[f] = dot(coefficient, held[f], ((1,), (1,))).astype(BF16)
        modes_copy(f).start()
        store(f).start()
        energy_out[pl.ds(f, 1), :] = jnp.sum(
            jnp.where(diagonal, basis[2 * KMAX :], 0.0), axis=0, keepdims=True
        )[:, :KMAX]
        weighted = modes[f, :, pl.ds(mine, part)].astype(F32) * weight[:, pl.ds(mine, part)]
        high, low = split(weighted)
        scaled[0, f] = high
        scaled[1, f] = low
        return carry

    lax.fori_loop(0, groups, modes_step, 0)

    def modes_wait(f, carry):
        modes_copy(f).wait_recv()
        return carry

    partner_copy.wait()
    lax.fori_loop(0, groups, modes_wait, 0)
    wide = groups * 2 * KMAX
    psi = mirrored[...].reshape(wide, part)
    cross = dot(scaled[0].reshape(wide, part), psi, ((1,), (1,)))
    cross = (cross + dot(scaled[1].reshape(wide, part), psi, ((1,), (1,)))) / total
    spread = functools.partial(jnp.concatenate, axis=1)
    copies = wide // 128
    partials[0] = choose(cross, spread([partners[0]] * copies), groups)
    partials[1] = choose(cross.T, spread([partners[1]] * copies), groups)

    def part_copy(side, source, peer):
        across = opposite if side else band
        return pltpu.make_async_remote_copy(
            src_ref=partials.at[side], dst_ref=arrived.at[side, source],
            send_sem=part_send.at[side, peer], recv_sem=part_recv.at[side, source],
            device_id=(across, peer), device_id_type=MESH,
        )

    for apart in range(n_space):
        peer = lax.rem(me + apart, n_space)
        part_copy(1, me, peer).start()
        if apart:
            part_copy(0, me, peer).start()

    def drain(f, carry):
        modes_copy(f).wait_send()
        store(f).wait()
        return carry

    lax.fori_loop(0, groups, drain, 0)
    for apart in range(1, n_space):
        peer = lax.rem(me + apart, n_space)
        basis_copy(me, peer).wait_send()
        for slot in range(own):
            gram_copy(peer * own + slot, chip).wait_send()

    result = partials[0]
    for apart in range(n_space):
        peer = lax.rem(me + apart, n_space)
        part_copy(1, peer, peer).wait()
        result = result + arrived[1, peer]
        if apart:
            part_copy(0, peer, peer).wait()
            result = result + arrived[0, peer]
    for f in range(groups):
        for kind in range(2):
            start = (2 * f + kind) * KMAX
            coherence_out[f, kind] = result[:, start : start + KMAX]


def on_device(n_freq, n_space, spectra, weight, partner, counts):
    groups, points, width = spectra.shape
    half = width // 2
    own = groups // n_space
    rows = 2 * KMAX
    wide = groups * rows
    dma = pltpu.SemaphoreType.DMA
    vmem = pl.BlockSpec(memory_space=pltpu.VMEM)
    smem = pl.BlockSpec(memory_space=pltpu.SMEM)
    hbm = pl.BlockSpec(memory_space=pltpu.HBM)
    modes, energy, coherence = pl.pallas_call(
        functools.partial(kernel, n_freq, n_space),
        out_shape=(
            jax.ShapeDtypeStruct((groups, rows, points), BF16),
            jax.ShapeDtypeStruct((groups, KMAX), F32),
            jax.ShapeDtypeStruct((groups, 2, KMAX, KMAX), F32),
        ),
        in_specs=[hbm, vmem, smem, smem],
        out_specs=(hbm, vmem, vmem),
        scratch_shapes=[
            pltpu.VMEM((groups, points, width), BF16),
            pltpu.VMEM((points, 128), F32),
            pltpu.VMEM((groups, half, half), F32),
            pltpu.VMEM((groups, half, half), F32),
            pltpu.VMEM((n_space // 2, own, half, half), F32),
            pltpu.VMEM((groups, 3 * KMAX, half), F32),
            pltpu.VMEM((groups, rows, points), BF16),
            pltpu.VMEM((groups, rows, points // 2), BF16),
            pltpu.VMEM((2, groups, rows, points // 2), BF16),
            pltpu.VMEM((2, groups, 128), jnp.int32),
            pltpu.VMEM((2, KMAX, wide), F32),
            pltpu.VMEM((2, n_space, KMAX, wide), F32),
            dma((groups,)),
            dma((groups,)),
            dma((groups,)),
            dma((n_space // 2, own)),
            dma((groups,)),
            dma((n_space,)),
            dma((n_space,)),
            dma((groups,)),
            dma((groups,)),
            dma(()),
            dma(()),
            dma((2, n_space)),
            dma((2, n_space)),
        ],
        compiler_params=pltpu.CompilerParams(
            collective_id=0, has_side_effects=True, vmem_limit_bytes=60 * 1024 * 1024
        ),
    )(spectra, weight.reshape(1, points), partner, counts)
    return modes, energy, coherence


def solution(mesh):
    in_specs = (P("freq", "space", None), P("space"), P("freq"), P("freq"))
    out_specs = (P("freq", None, "space"), P("freq", None), P("freq", None, None, None))
    return jax.shard_map(
        functools.partial(on_device, mesh.shape["freq"], mesh.shape["space"]),
        mesh=mesh,
        in_specs=in_specs,
        out_specs=out_specs,
        check_vma=False,
    )
```
